32 devices in a mesh: dp: 2 (over x), col: 4 (over z), row: 4 (over y, core).
Axes of the slice: x: 2, y: 2, z: 4, core: 2. Of those that a mesh axis runs over, the one named last changes fastest.
Arguments:
- seq_in: bfloat16 [16, 128, 5760], P(None, 'dp', 'row'), parts along dimension 1
- w_in1: bfloat16 [5760, 23040], P('row', 'col')
- w_rec1: bfloat16 [5760, 23040], P('row', 'col')
- b_gate1: float32 [23040], P(('col', 'row'))
- w_in2: bfloat16 [5760, 23040], P('row', 'col')
- w_rec2: bfloat16 [5760, 23040], P('row', 'col')
- b_gate2: float32 [23040], P(('col', 'row'))
- h_init: float32 [2, 128, 5760], P(None, 'dp', 'row'), parts along dimension 1
- c_init: float32 [2, 128, 5760], P(None, 'dp', 'row'), parts along dimension 1
Outputs:
- output 1: bfloat16 [16, 128, 5760], P(None, 'dp', ('row', 'col')), parts along dimension 1
- output 2: float32 [128, 5760], P('dp', ('row', 'col')), parts along dimension 0
- output 3: float32 [128, 5760], P('dp', ('row', 'col')), parts along dimension 0
There are 2 independent parts. The reference program is written for one: setup_inputs(seed, part) draws one part's arguments, and reference() takes and returns one part's arrays. A program takes and returns all parts, laid end to end along the dimension named above; an argument that names none is the same for every part.
All inputs are finite; a program needn't handle non-finite values.
Results may differ from the reference program's by a relative error of at most 0.00285702.
Values are sent between devices in bfloat16 or wider.
A program may use at most 1 GiB of HBM per device.

```python
import jax
import jax.numpy as jnp
from jax import lax

HIDDEN = 5760
TIME_STEPS = 16
GROUP_BATCH = 64
ROW_SPLIT = 4
COL_SPLIT = 4


def forget_offset():
    unit_dev = HIDDEN // (ROW_SPLIT * COL_SPLIT)
    gate_index = (jnp.arange(4 * HIDDEN) // unit_dev) % 4
    return jnp.where(gate_index == 1, 1.0, 0.0).astype(jnp.float32)


def setup_inputs(seed: int = 0, part: int = 0) -> dict:
    shared_keys = jax.random.split(jax.random.key(seed), 6)
    part_keys = jax.random.split(jax.random.fold_in(jax.random.key(seed + 1), part), 3)
    w_scale = HIDDEN ** -0.5

    def weight_draw(rng_key):
        return (w_scale * jax.random.normal(rng_key, (HIDDEN, 4 * HIDDEN), jnp.float32)).astype(jnp.bfloat16)

    def bias_draw(rng_key):
        return 0.5 * jax.random.normal(rng_key, (4 * HIDDEN,), jnp.float32) + forget_offset()

    return {
        "seq_in": jax.random.normal(part_keys[0], (TIME_STEPS, GROUP_BATCH, HIDDEN), jnp.float32).astype(jnp.bfloat16),
        "w_in1": weight_draw(shared_keys[0]),
        "w_rec1": weight_draw(shared_keys[1]),
        "b_gate1": bias_draw(shared_keys[2]),
        "w_in2": weight_draw(shared_keys[3]),
        "w_rec2": weight_draw(shared_keys[4]),
        "b_gate2": bias_draw(shared_keys[5]),
        "h_init": 0.5 * jax.random.normal(part_keys[1], (2, GROUP_BATCH, HIDDEN), jnp.float32),
        "c_init": 1.2 * jax.random.normal(part_keys[2], (2, GROUP_BATCH, HIDDEN), jnp.float32),
    }


def lstm_layer(in_seq, w_in, w_rec, b_gate, h_first, c_first):
    batch_rows = in_seq.shape[1]
    unit_dev = HIDDEN // (ROW_SPLIT * COL_SPLIT)

    def to_packed(flat_state):
        return flat_state.reshape(batch_rows, ROW_SPLIT, COL_SPLIT, unit_dev).transpose(0, 2, 1, 3)

    def to_plain(packed_state):
        return packed_state.transpose(0, 2, 1, 3).reshape(batch_rows, HIDDEN)

    def lstm_step(carry_in, in_step):
        h_prev, c_prev = carry_in
        z_cols = jnp.dot(in_step, w_in, preferred_element_type=jnp.float32) + b_gate
        z_cols = z_cols + jnp.dot(h_prev, w_rec, preferred_element_type=jnp.float32)
        z_pack = z_cols.reshape(batch_rows, COL_SPLIT, ROW_SPLIT, 4, unit_dev)
        in_gate = jax.nn.sigmoid(z_pack[:, :, :, 0])
        forget = jax.nn.sigmoid(z_pack[:, :, :, 1])
        cell_in = jnp.tanh(z_pack[:, :, :, 2])
        out_gate = jax.nn.sigmoid(z_pack[:, :, :, 3])
        c_new = forget * c_prev + in_gate * cell_in
        h_new = to_plain(out_gate * jnp.tanh(c_new)).astype(jnp.bfloat16)
        return (h_new, c_new), h_new

    carry_out, h_seq = lax.scan(lstm_step, (h_first.astype(jnp.bfloat16), to_packed(c_first)), in_seq)
    return h_seq, to_plain(carry_out[1])


def reference(seq_in, w_in1, w_rec1, b_gate1, w_in2, w_rec2, b_gate2, h_init, c_init):
    h1_seq, c1_last = lstm_layer(seq_in, w_in1, w_rec1, b_gate1, h_init[0], c_init[0])
    h2_seq, c2_last = lstm_layer(h1_seq, w_in2, w_rec2, b_gate2, h_init[1], c_init[1])
    return h2_seq, c1_last, c2_last
```

```python
import jax
import jax.numpy as jnp
from jax import lax
from jax.experimental import pallas as pl
from jax.experimental.pallas import tpu as pltpu
from jax.sharding import PartitionSpec as P

MESH = pl.DeviceIdType.MESH
F32 = jnp.float32
BF16 = jnp.bfloat16
LANES = 128
ROW_CHUNK = 16


def lstm_kernel(steps, batch, n, rows_dev, cols_dev, width, pad_n,
                pin_hbm, w1_hbm, w2i_hbm, w2r_hbm, h0_ref, c0_ref, bias_ref,
                h2_out, c1_out, c2_out,
                w1, w2i, w2r, pin, hrow, cell, hblk, zb, rd, yr,
                w_sem, pin_sem, d_send, d_recv, y_send, y_recv, a_send, a_recv):
    row = lax.axis_index("row")
    col = lax.axis_index("col")
    core = lax.rem(row, 2)
    ypos = row // 2
    sibling = ypos * 2 + (1 - core)
    across = (1 - ypos) * 2 + core
    owners = ((1 - ypos) * 2 + (1 - core), across, sibling, row)
    tile_step = (n * 4) // LANES * LANES

    w_copies = [pltpu.make_async_copy(src, dst, w_sem.at[j])
                for j, (src, dst) in enumerate(((w1_hbm, w1), (w2i_hbm, w2i), (w2r_hbm, w2r)))]
    for cp in w_copies:
        cp.start()

    def pin_copy(step):
        slot = lax.rem(step, 2)
        return pltpu.make_async_copy(pin_hbm.at[step], pin.at[slot], pin_sem.at[slot])

    pin_copy(0).start()

    barrier = pltpu.get_barrier_semaphore()
    for peer_row in (sibling, across):
        pl.semaphore_signal(barrier, inc=1, device_id={"row": peer_row}, device_id_type=MESH)
    for j in (1, 2, 3):
        pl.semaphore_signal(barrier, inc=1, device_id={"col": lax.rem(col + j, 4)}, device_id_type=MESH)

    for layer in range(2):
        hrow[layer] = h0_ref[layer]
        cell[layer] = c0_ref[layer]
    pl.semaphore_wait(barrier, 5)

    def d2d(layer, par, half):
        return pltpu.make_async_remote_copy(
            src_ref=zb.at[layer, 2 * half], dst_ref=rd.at[layer, par, half],
            send_sem=d_send.at[layer, half], recv_sem=d_recv.at[layer, par, half],
            device_id={"row": sibling}, device_id_type=MESH)

    def ysum(layer, par):
        return pltpu.make_async_remote_copy(
            src_ref=zb.at[layer, 1], dst_ref=yr.at[layer, par],
            send_sem=y_send.at[layer], recv_sem=y_recv.at[layer, par],
            device_id={"row": across}, device_id_type=MESH)

    def gather(layer, par, j, src_col):
        return pltpu.make_async_remote_copy(
            src_ref=hblk.at[layer, par, src_col], dst_ref=hblk.at[layer, par, src_col],
            send_sem=a_send.at[layer, j], recv_sem=a_recv.at[layer, par, src_col],
            device_id={"col": lax.rem(col + j, 4)}, device_id_type=MESH)

    def gather_start(layer, par):
        for j in (1, 2, 3):
            gather(layer, par, j, col).start()

    def gather_wait_send(layer, par):
        for j in (1, 2, 3):
            gather(layer, par, j, col).wait_send()

    def assemble(layer, par):
        for j in (1, 2, 3):
            gather(layer, par, j, lax.rem(col + j, 4)).wait_recv()
        for q in range(0, batch, ROW_CHUNK):
            rows = pl.ds(q, ROW_CHUNK)
            tiles = [None] * (width // LANES)
            for k in range(4):
                first, off = (k * n) // LANES, (k * n) % LANES
                block = hblk[layer, par, k, rows, :].astype(F32)
                if off:
                    block = jnp.concatenate([block, jnp.zeros((ROW_CHUNK, LANES), F32)], axis=1)
                    block = pltpu.roll(block, off, axis=1)
                for t in range(block.shape[1] // LANES):
                    piece = block[:, t * LANES:(t + 1) * LANES]
                    held = tiles[first + t]
                    tiles[first + t] = piece if held is None else held + piece
            for t, piece in enumerate(tiles):
                hrow[layer, rows, t * LANES:(t + 1) * LANES] = piece.astype(BF16)

    def columns(i):
        return pl.ds(pl.multiple_of(owners[i] * tile_step, LANES), width)

    def dot_block(layer, weights, i):
        return jnp.dot(hrow[layer, :, :rows_dev], weights[:, columns(i)], preferred_element_type=F32)

    def reduce_first(layer, par):
        d2d(layer, par, 0).wait_recv()
        zb[layer, 1] = zb[layer, 1] + rd[layer, par, 0]
        ysum(layer, par).start()

    def cell_update(layer, par):
        d2d(layer, par, 1).wait_recv()
        ysum(layer, par).wait_recv()
        span = pad_n + LANES
        lane = lax.broadcasted_iota(jnp.int32, (ROW_CHUNK, pad_n), 1)
        start0 = row * (4 * n - tile_step)
        for q in range(0, batch, ROW_CHUNK):
            rows = pl.ds(q, ROW_CHUNK)
            gates = []
            for m in range(4):
                start = start0 + m * n
                tile = jnp.minimum(start // LANES, (width - span) // LANES)
                shift = start - tile * LANES
                at = pl.ds(pl.multiple_of(tile * LANES, LANES), span)
                z = zb[layer, 3, rows, at] + rd[layer, par, 1, rows, at] + yr[layer, par, rows, at]
                z = pltpu.roll(z, span - shift, axis=1)[:, :pad_n]
                gates.append(z + bias_ref[layer, m:m + 1, :])
            c_new = (jax.nn.sigmoid(gates[1]) * cell[layer, rows, :]
                     + jax.nn.sigmoid(gates[0]) * jnp.tanh(gates[2]))
            cell[layer, rows, :] = c_new
            h_new = jax.nn.sigmoid(gates[3]) * jnp.tanh(c_new)
            hblk[layer, par, col, rows, :] = jnp.where(lane < n, h_new, 0.0).astype(BF16)

    def wait_sum_sends(layer, par):
        d2d(layer, par, 0).wait_send()
        d2d(layer, par, 1).wait_send()
        ysum(layer, par).wait_send()

    def step_body(s, carry):
        par = lax.rem(s, 2)
        prev = 1 - par

        @pl.when(s > 0)
        def _():
            assemble(0, prev)

        @pl.when(s < steps)
        def _():
            pin_copy(s).wait()

            @pl.when(s + 1 < steps)
            def _():
                pin_copy(s + 1).start()

            @pl.when(s == 0)
            def _():
                w_copies[0].wait()

            for i in range(4):
                zb[0, i] = dot_block(0, w1, i) + pin[par, :, columns(i)]
                if i % 2 == 0:
                    d2d(0, par, i // 2).start()
                if i == 2:
                    reduce_first(0, par)

        @pl.when(s == 1)
        def _():
            w_copies[1].wait()
            w_copies[2].wait()

        @pl.when(s >= 2)
        def _():
            @pl.when(s >= 3)
            def _():
                gather_wait_send(1, prev)

            cell_update(1, par)
            h2_out[s - 2] = hblk[1, par, col, :, :n]
            gather_start(1, par)
            wait_sum_sends(1, par)

        @pl.when(s >= 1)
        def _():
            for i in range(4):
                zb[1, i] = dot_block(0, w2i, i)

            @pl.when(s >= 2)
            def _():
                assemble(1, par)

            for i in range(4):
                zb[1, i] = zb[1, i] + dot_block(1, w2r, i)
                if i % 2 == 0:
                    d2d(1, prev, i // 2).start()
                if i == 2:
                    reduce_first(1, prev)

        @pl.when(s < steps)
        def _():
            @pl.when(s >= 1)
            def _():
                gather_wait_send(0, prev)

            cell_update(0, par)
            gather_start(0, par)
            wait_sum_sends(0, par)

        return carry

    lax.fori_loop(0, steps + 1, step_body, 0)

    last = (steps - 1) % 2
    gather_wait_send(1, 1 - last)
    gather_wait_send(0, last)
    cell_update(1, last)
    h2_out[steps - 1] = hblk[1, last, col, :, :n]
    wait_sum_sends(1, last)
    c1_out[...] = cell[0, :, :n]
    c2_out[...] = cell[1, :, :n]


def solution(mesh):
    def local_program(seq_in, w_in1, w_rec1, b_gate1, w_in2, w_rec2, b_gate2, h_init, c_init):
        steps, batch, rows_dev = seq_in.shape
        cols_dev = w_in1.shape[1]
        n = b_gate1.shape[0] // 4
        pad_n = -(-n // LANES) * LANES
        width = -(-rows_dev // LANES) * LANES

        pin = jnp.dot(seq_in.reshape(steps * batch, rows_dev), w_in1, preferred_element_type=F32)
        pin = pin.reshape(steps, batch, cols_dev)
        h0 = jnp.pad(h_init.astype(BF16), ((0, 0), (0, 0), (0, width - rows_dev)))
        c0 = lax.dynamic_slice_in_dim(c_init, lax.axis_index("col") * n, n, axis=2)
        c0 = jnp.pad(c0, ((0, 0), (0, 0), (0, pad_n - n)))
        bias = jnp.stack([b_gate1, b_gate2]).reshape(2, 4, n)
        bias = jnp.pad(bias, ((0, 0), (0, 0), (0, pad_n - n)))

        def kernel(*refs):
            lstm_kernel(steps, batch, n, rows_dev, cols_dev, width, pad_n, *refs)

        hbm = pl.BlockSpec(memory_space=pl.ANY)
        vmem = pl.BlockSpec(memory_space=pltpu.VMEM)
        dma = pltpu.SemaphoreType.DMA
        return pl.pallas_call(
            kernel,
            name="lstm_grid",
            out_shape=(jax.ShapeDtypeStruct((steps, batch, n), BF16),
                       jax.ShapeDtypeStruct((batch, n), F32),
                       jax.ShapeDtypeStruct((batch, n), F32)),
            in_specs=[hbm] * 4 + [vmem] * 3,
            out_specs=(vmem, vmem, vmem),
            scratch_shapes=[
                pltpu.VMEM((rows_dev, cols_dev), BF16),
                pltpu.VMEM((rows_dev, cols_dev), BF16),
                pltpu.VMEM((rows_dev, cols_dev), BF16),
                pltpu.VMEM((2, batch, cols_dev), F32),
                pltpu.VMEM((2, batch, width), BF16),
                pltpu.VMEM((2, batch, pad_n), F32),
                pltpu.VMEM((2, 2, 4, batch, pad_n), BF16),
                pltpu.VMEM((2, 4, batch, width), F32),
                pltpu.VMEM((2, 2, 2, batch, width), F32),
                pltpu.VMEM((2, 2, batch, width), F32),
                dma((3,)), dma((2,)),
                dma((2, 2)), dma((2, 2, 2)),
                dma((2,)), dma((2, 2)),
                dma((2, 3 + 1)), dma((2, 2, 4)),
            ],
            compiler_params=pltpu.CompilerParams(
                collective_id=0, has_side_effects=True, vmem_limit_bytes=67043328),
        )(pin, w_rec1, w_in2, w_rec2, h0, c0, bias)

    row_spec = P(None, "dp", "row")
    weight_spec = P("row", "col")
    bias_spec = P(("col", "row"))
    seq_out_spec = P(None, "dp", ("row", "col"))
    cell_out_spec = P("dp", ("row", "col"))
    return jax.shard_map(
        local_program,
        mesh=mesh,
        in_specs=(row_spec, weight_spec, weight_spec, bias_spec, weight_spec, weight_spec, bias_spec, row_spec, row_spec),
        out_specs=(seq_out_spec, cell_out_spec, cell_out_spec),
        check_vma=False,
    )
```

```python
import jax
import jax.numpy as jnp
from jax import lax
from jax.experimental import pallas as pl
from jax.experimental.pallas import tpu as pltpu
from jax.sharding import PartitionSpec as P

MESH = pl.DeviceIdType.MESH
F32 = jnp.float32
BF16 = jnp.bfloat16
LANES = 128
ROW_CHUNK = 8
PIECES = ((0, 32), (32, 24), (56, 8))
STRIP = 512


def lstm_kernel(steps, batch, n, rows_dev, cols_dev, width, pad_n,
                pin_hbm, w1_hbm, w2i_hbm, w2r_hbm, h0_ref, c0_ref, bias_ref,
                h2_out, c1_out, c2_out,
                w1, w2i, w2r, pin, cell, hblk, zb, rd, yr,
                w_sem, pin_sem, d_send, d_recv, y_send, y_recv, a_send, a_recv):
    row = lax.axis_index("row")
    col = lax.axis_index("col")
    core = lax.rem(row, 2)
    ypos = row // 2
    sibling = ypos * 2 + (1 - core)
    across = (1 - ypos) * 2 + core
    owners = ((1 - ypos) * 2 + (1 - core), across, sibling, row)
    tile_step = (n * 4) // LANES * LANES
    strips = tuple(range(0, width, STRIP))

    w_copies = [pltpu.make_async_copy(src, dst, w_sem.at[j])
                for j, (src, dst) in enumerate(((w1_hbm, w1), (w2i_hbm, w2i), (w2r_hbm, w2r)))]
    for cp in w_copies:
        cp.start()

    def pin_copy(step):
        slot = lax.rem(step, 2)
        return pltpu.make_async_copy(pin_hbm.at[step], pin.at[slot], pin_sem.at[slot])

    pin_copy(0).start()

    barrier = pltpu.get_barrier_semaphore()
    for peer_row in (sibling, across):
        pl.semaphore_signal(barrier, inc=1, device_id={"row": peer_row}, device_id_type=MESH)
    for j in (1, 2, 3):
        pl.semaphore_signal(barrier, inc=1, device_id={"col": lax.rem(col + j, 4)}, device_id_type=MESH)

    for layer in range(2):
        hblk[layer, 1] = h0_ref[layer]
        cell[layer] = c0_ref[layer]
    pl.semaphore_wait(barrier, 5)

    def d2d(layer, par, j):
        if j < len(strips):
            src, dst = zb.at[layer, 0, :, pl.ds(strips[j], STRIP)], rd.at[layer, par, 0, :, pl.ds(strips[j], STRIP)]
        else:
            src, dst = zb.at[layer, 2], rd.at[layer, par, 1]
        return pltpu.make_async_remote_copy(
            src_ref=src, dst_ref=dst, send_sem=d_send.at[layer, j], recv_sem=d_recv.at[layer, par, j],
            device_id={"row": sibling}, device_id_type=MESH)

    def ysum(layer, par, j):
        if j < len(strips):
            at = (pl.ds(*PIECES[0]), pl.ds(strips[j], STRIP))
        else:
            at = (pl.ds(*PIECES[j - len(strips) + 1]), slice(None))
        return pltpu.make_async_remote_copy(
            src_ref=zb.at[(layer, 1) + at], dst_ref=yr.at[(layer, par) + at],
            send_sem=y_send.at[layer, j], recv_sem=y_recv.at[layer, par, j],
            device_id={"row": across}, device_id_type=MESH)

    y_copies = len(strips) + len(PIECES) - 1

    far = 3 * (1 - col // 2)
    near = 1 + lax.rem(col, 2)
    others = (far, 6 - col - far - near, near)

    def gather(layer, piece, par, j, src_col):
        at = (layer, par, src_col, pl.ds(*PIECES[piece]))
        return pltpu.make_async_remote_copy(
            src_ref=hblk.at[at], dst_ref=hblk.at[at],
            send_sem=a_send.at[layer, piece, j], recv_sem=a_recv.at[layer, par, piece, src_col],
            device_id={"col": others[j]}, device_id_type=MESH)

    def gather_start(layer, piece, par):
        for j in range(3):
            gather(layer, piece, par, j, col).start()

    def gather_wait_send(layer, par):
        for piece in range(len(PIECES)):
            for j in range(3):
                gather(layer, piece, par, j, col).wait_send()

    def gather_wait(layer, par):
        for piece in range(len(PIECES)):
            for j in range(3):
                gather(layer, piece, par, j, others[j]).wait_recv()

    def columns(i, start, size):
        return pl.ds(pl.multiple_of(owners[i] * tile_step + start, LANES), size)

    def dot_block(layer, par, weights, i, start, size):
        total = None
        for k in range(4):
            part = jnp.dot(hblk[layer, par, k, :, :n], weights[k * n:(k + 1) * n, columns(i, start, size)],
                           preferred_element_type=F32)
            total = part if total is None else total + part
        return total

    def send_sums(layer, par, block, between):
        def strip(i, j):
            zb[layer, i, :, strips[j]:strips[j] + STRIP] = block(i, strips[j], STRIP)

        for j in range(len(strips)):
            strip(0, j)
            d2d(layer, par, j).start()
        for j in range(len(strips)):
            strip(1, j)
            d2d(layer, par, j).wait_recv()
            at = slice(strips[j], strips[j] + STRIP)
            zb[layer, 1, :, at] = zb[layer, 1, :, at] + rd[layer, par, 0, :, at]
            ysum(layer, par, j).start()
        for j in range(len(strips), y_copies):
            ysum(layer, par, j).start()
        zb[layer, 2] = block(2, 0, width)
        d2d(layer, par, len(strips)).start()
        between()
        zb[layer, 3] = block(3, 0, width)

    def cell_update(layer, piece, par, step):
        if piece == 0:
            d2d(layer, par, len(strips)).wait_recv()
            for j in range(len(strips)):
                ysum(layer, par, j).wait_recv()
        else:
            ysum(layer, par, len(strips) + piece - 1).wait_recv()
        span = pad_n + LANES
        lane = lax.broadcasted_iota(jnp.int32, (ROW_CHUNK, pad_n), 1)
        start0 = row * (4 * n - tile_step)
        first, size = PIECES[piece]
        for q in range(first, first + size, ROW_CHUNK):
            rows = pl.ds(q, ROW_CHUNK)
            gates = []
            for m in range(4):
                start = start0 + m * n
                tile = jnp.minimum(start // LANES, (width - span) // LANES)
                shift = start - tile * LANES
                at = pl.ds(pl.multiple_of(tile * LANES, LANES), span)
                z = zb[layer, 3, rows, at] + rd[layer, par, 1, rows, at] + yr[layer, par, rows, at]
                z = pltpu.roll(z, span - shift, axis=1)[:, :pad_n]
                gates.append(z + bias_ref[layer, m:m + 1, :])
            c_new = (jax.nn.sigmoid(gates[1]) * cell[layer, rows, :]
                     + jax.nn.sigmoid(gates[0]) * jnp.tanh(gates[2]))
            cell[layer, rows, :] = c_new
            h_new = jnp.where(lane < n, jax.nn.sigmoid(gates[3]) * jnp.tanh(c_new), 0.0).astype(BF16)
            hblk[layer, par, col, rows, :] = h_new
            if layer == 1:
                h2_out[step, rows, :] = h_new[:, :n]

    def wait_sum_sends(layer, par):
        for j in range(len(strips) + 1):
            d2d(layer, par, j).wait_send()
        for j in range(y_copies):
            ysum(layer, par, j).wait_send()

    def finish(layer, piece, par, step, first):
        if piece == 0:
            @pl.when(jnp.logical_not(first))
            def _():
                gather_wait_send(layer, 1 - par)

        cell_update(layer, piece, par, step)
        gather_start(layer, piece, par)
        if piece == len(PIECES) - 1:
            wait_sum_sends(layer, par)

    def step_body(s, carry):
        par = lax.rem(s, 2)
        prev = 1 - par

        def finish_two():
            @pl.when(s >= 2)
            def _():
                finish(1, 1, par, s - 2, s == 2)

        @pl.when(s > 0)
        def _():
            gather_wait(0, prev)

        @pl.when(s < steps)
        def _():
            pin_copy(s).wait()

            @pl.when(s + 1 < steps)
            def _():
                pin_copy(s + 1).start()

            @pl.when(s == 0)
            def _():
                w_copies[0].wait()

            send_sums(0, par, lambda i, start, size: dot_block(0, prev, w1, i, start, size)
                      + pin[par, :, columns(i, start, size)], finish_two)

        @pl.when(s == steps)
        def _():
            finish_two()

        @pl.when(s >= 2)
        def _():
            finish(1, 2, par, s - 2, s == 2)

        @pl.when(s == 1)
        def _():
            w_copies[1].wait()
            w_copies[2].wait()

        @pl.when(s >= 1)
        def _():
            for i in range(4):
                zb[1, i] = dot_block(0, prev, w2i, i, 0, width)

        @pl.when(s < steps)
        def _():
            finish(0, 0, par, s, s == 0)

        def finish_one():
            @pl.when(s < steps)
            def _():
                finish(0, 1, par, s, s == 0)

        @pl.when(s >= 1)
        def _():
            @pl.when(s >= 2)
            def _():
                gather_wait(1, par)

            send_sums(1, prev, lambda i, start, size: zb[1, i, :, start:start + size]
                      + dot_block(1, par, w2r, i, start, size), finish_one)

        @pl.when(s == 0)
        def _():
            finish_one()

        @pl.when(s < steps)
        def _():
            finish(0, 2, par, s, s == 0)

        @pl.when(jnp.logical_and(s >= 1, s < steps))
        def _():
            finish(1, 0, prev, s - 1, s == 1)

        return carry

    lax.fori_loop(0, steps + 1, step_body, 0)

    last = (steps - 1) % 2
    gather_wait_send(1, 1 - last)
    gather_wait_send(0, last)
    for piece in range(len(PIECES)):
        cell_update(1, piece, last, steps - 1)
    wait_sum_sends(1, last)
    c1_out[...] = cell[0, :, :n]
    c2_out[...] = cell[1, :, :n]


def solution(mesh):
    def local_program(seq_in, w_in1, w_rec1, b_gate1, w_in2, w_rec2, b_gate2, h_init, c_init):
        steps, batch, rows_dev = seq_in.shape
        cols_dev = w_in1.shape[1]
        n = b_gate1.shape[0] // 4
        pad_n = -(-n // LANES) * LANES
        width = -(-rows_dev // LANES) * LANES

        pin = jnp.dot(seq_in.reshape(steps * batch, rows_dev), w_in1, preferred_element_type=F32)
        pin = pin.reshape(steps, batch, cols_dev)
        h0 = h_init.astype(BF16).reshape(2, batch, 4, n).transpose(0, 2, 1, 3)
        h0 = jnp.pad(h0, ((0, 0), (0, 0), (0, 0), (0, pad_n - n)))
        c0 = lax.dynamic_slice_in_dim(c_init, lax.axis_index("col") * n, n, axis=2)
        c0 = jnp.pad(c0, ((0, 0), (0, 0), (0, pad_n - n)))
        bias = jnp.stack([b_gate1, b_gate2]).reshape(2, 4, n)
        bias = jnp.pad(bias, ((0, 0), (0, 0), (0, pad_n - n)))

        def kernel(*refs):
            lstm_kernel(steps, batch, n, rows_dev, cols_dev, width, pad_n, *refs)

        hbm = pl.BlockSpec(memory_space=pl.ANY)
        vmem = pl.BlockSpec(memory_space=pltpu.VMEM)
        dma = pltpu.SemaphoreType.DMA
        strips, pieces = width // STRIP, len(PIECES)
        return pl.pallas_call(
            kernel,
            name="lstm_grid",
            out_shape=(jax.ShapeDtypeStruct((steps, batch, n), BF16),
                       jax.ShapeDtypeStruct((batch, n), F32),
                       jax.ShapeDtypeStruct((batch, n), F32)),
            in_specs=[hbm] * 4 + [vmem] * 3,
            out_specs=(vmem, vmem, vmem),
            scratch_shapes=[
                pltpu.VMEM((rows_dev, cols_dev), BF16),
                pltpu.VMEM((rows_dev, cols_dev), BF16),
                pltpu.VMEM((rows_dev, cols_dev), BF16),
                pltpu.VMEM((2, batch, cols_dev), F32),
                pltpu.VMEM((2, batch, pad_n), F32),
                pltpu.VMEM((2, 2, 4, batch, pad_n), BF16),
                pltpu.VMEM((2, 4, batch, width), F32),
                pltpu.VMEM((2, 2, 2, batch, width), F32),
                pltpu.VMEM((2, 2, batch, width), F32),
                dma((3,)), dma((2,)),
                dma((2, strips + 1)), dma((2, 2, strips + 1)),
                dma((2, strips + pieces - 1)), dma((2, 2, strips + pieces - 1)),
                dma((2, pieces, 3)), dma((2, 2, pieces, 4)),
            ],
            compiler_params=pltpu.CompilerParams(
                collective_id=0, has_side_effects=True, vmem_limit_bytes=67043328),
        )(pin, w_rec1, w_in2, w_rec2, h0, c0, bias)

    row_spec = P(None, "dp", "row")
    weight_spec = P("row", "col")
    bias_spec = P(("col", "row"))
    seq_out_spec = P(None, "dp", ("row", "col"))
    cell_out_spec = P("dp", ("row", "col"))
    return jax.shard_map(
        local_program,
        mesh=mesh,
        in_specs=(row_spec, weight_spec, weight_spec, bias_spec, weight_spec, weight_spec, bias_spec, row_spec, row_spec),
        out_specs=(seq_out_spec, cell_out_spec, cell_out_spec),
        check_vma=False,
    )
```

```python
import jax
import jax.numpy as jnp
from jax import lax
from jax.experimental import pallas as pl
from jax.experimental.pallas import tpu as pltpu
from jax.sharding import PartitionSpec as P

MESH = pl.DeviceIdType.MESH
F32 = jnp.float32
BF16 = jnp.bfloat16
LANES = 128
ROW_CHUNK = 8
PIECES = ((0, 32), (32, 24), (56, 8))
STRIPS = (((128, 512),), ((640, 512),), ((1152, 384), (0, 128)))
D2D_LANES = tuple(part for strip in STRIPS for part in strip)
GROUP = 4


def lstm_kernel(steps, batch, n, rows_dev, cols_dev, width, pad_n,
                seq_hbm, w1i_hbm, w1_hbm, w2i_hbm, w2r_hbm, h0_ref, c0_ref, b1_ref, b2_ref,
                h2_out, c1_out, c2_out, pin_hbm,
                w1, w2i, w2r, xbuf, pin, cell, bias, hblk, zb, rd, yr, es, er,
                w_sem, wi_sem, x_sem, st_sem, pin_sem, d_send, d_recv, y_send, y_recv, e_send, e_recv, a_send, a_recv):
    row = lax.axis_index("row")
    col = lax.axis_index("col")
    core = lax.rem(row, 2)
    ypos = row // 2
    sibling = ypos * 2 + (1 - core)
    across = (1 - ypos) * 2 + core
    owners = ((1 - ypos) * 2 + (1 - core), across, sibling, row)
    tile_step = (n * 4) // LANES * LANES
    edge = width - LANES
    lane = lax.broadcasted_iota(jnp.int32, (ROW_CHUNK, LANES), 1)

    w_copies = [pltpu.make_async_copy(src, dst, w_sem.at[j])
                for j, (src, dst) in enumerate(((w1_hbm, w1), (w2i_hbm, w2i), (w2r_hbm, w2r)))]

    spans = 4

    def span_at(j):
        return pl.ds(pl.multiple_of(jnp.minimum(j * width, cols_dev - width), LANES), width)

    def w1i_copy(j):
        at = pl.ds(j * width, min(width, cols_dev - j * width))
        return pltpu.make_async_copy(w1i_hbm.at[:, at], w2r.at[:, at], wi_sem.at[j])

    def x_copy(g):
        return pltpu.make_async_copy(seq_hbm.at[pl.ds(g * GROUP, GROUP)], xbuf.at[g % 2], x_sem.at[g % 2])

    def stage_copy(g, j, slot):
        src = zb.at[1] if slot == 0 else rd.at[1].reshape(GROUP, batch, width)
        return pltpu.make_async_copy(src, pin_hbm.at[pl.ds(g * GROUP, GROUP), :, span_at(j)], st_sem.at[slot])

    def project(g):
        x_copy(g).wait()
        if (g + 1) * GROUP < steps:
            x_copy(g + 1).start()

        def pair(jj, carry):
            for slot in range(2):
                j = 2 * jj + slot

                @pl.when(jj > 0)
                def _():
                    stage_copy(g, j - 2, slot).wait()

                z = jnp.dot(xbuf[g % 2].reshape(GROUP * batch, rows_dev), w2r[:, span_at(j)], preferred_element_type=F32)
                if slot == 0:
                    zb[1] = z.reshape(GROUP, batch, width)
                else:
                    rd[1] = z.reshape(2, 2, batch, width)
                    @pl.when(jj > 0)
                    def _():
                        stage_copy(g, j - 1, 0).wait()
                stage_copy(g, j, slot).start()
            return carry

        return pair

    def run_project(g):
        lax.fori_loop(0, spans // 2, project(g), 0)
        stage_copy(g, spans - 1, 1).wait()

    x_copy(0).start()
    for j in range(spans):
        w1i_copy(j).start()

    def pin_copy(step):
        slot = lax.rem(step, 2)
        return pltpu.make_async_copy(pin_hbm.at[step], pin.at[slot], pin_sem.at[slot])

    barrier = pltpu.get_barrier_semaphore()
    for peer_row in (sibling, across):
        pl.semaphore_signal(barrier, inc=1, device_id={"row": peer_row}, device_id_type=MESH)
    for j in (1, 2, 3):
        pl.semaphore_signal(barrier, inc=1, device_id={"col": lax.rem(col + j, 4)}, device_id_type=MESH)

    for layer in range(2):
        hblk[layer, 1, :, :, :n] = h0_ref[layer]
        cell[layer] = jnp.zeros((batch, pad_n), F32)
        cell[layer, :, :n] = c0_ref[layer]
        bias[layer] = jnp.zeros((8, pad_n), F32)
        bias[layer, :4, :n] = (b1_ref, b2_ref)[layer][...]
    first_pair = project(0)
    for jj in range(spans // 2):
        w1i_copy(2 * jj).wait()
        w1i_copy(2 * jj + 1).wait()
        first_pair(jj, 0)
        w_copies[jj].start()
    stage_copy(0, spans - 1, 1).wait()
    pin_copy(0).start()
    pl.semaphore_wait(barrier, 5)

    def d2d(layer, par, j):
        if j < len(D2D_LANES):
            at = pl.ds(*D2D_LANES[j])
            src, dst = zb.at[layer, 0, :, at], rd.at[layer, par, 0, :, at]
        else:
            src, dst = zb.at[layer, 2], rd.at[layer, par, 1]
        return pltpu.make_async_remote_copy(
            src_ref=src, dst_ref=dst, send_sem=d_send.at[layer, j], recv_sem=d_recv.at[layer, par, j],
            device_id={"row": sibling}, device_id_type=MESH)

    def ysum(layer, par, j):
        if j < len(STRIPS):
            at = (pl.ds(*PIECES[0]), pl.ds(*STRIPS[j][0]))
        else:
            at = (pl.ds(*PIECES[j - len(STRIPS) + 1]), pl.ds(LANES, edge))
        return pltpu.make_async_remote_copy(
            src_ref=zb.at[(layer, 1) + at], dst_ref=yr.at[(layer, par) + at],
            send_sem=y_send.at[layer, j], recv_sem=y_recv.at[layer, par, j],
            device_id={"row": across}, device_id_type=MESH)

    def yedge(layer, par, piece):
        return pltpu.make_async_remote_copy(
            src_ref=es.at[layer, piece], dst_ref=er.at[layer, par, piece],
            send_sem=e_send.at[layer, piece], recv_sem=e_recv.at[layer, par, piece],
            device_id={"row": across}, device_id_type=MESH)

    y_copies = len(STRIPS) + len(PIECES) - 1

    def pack_edges(layer, par):
        own = across * 32
        quarter = jnp.bitwise_and(jnp.right_shift(lane, 5) + 4 - across, 3)
        for piece, (first, size) in enumerate(PIECES):
            packed = None
            for g in range(size // ROW_CHUNK):
                rows = pl.ds(first + g * ROW_CHUNK, ROW_CHUNK)
                head = zb[layer, 1, rows, :LANES] + rd[layer, par, 0, rows, :LANES]
                tail = zb[layer, 1, rows, edge:] + rd[layer, par, 0, rows, edge:]
                zb[layer, 1, rows, edge:] = jnp.where(lane >= own, head, tail)
                moved = pltpu.roll(tail, 32 * g, axis=1) if g else tail
                packed = moved if packed is None else jnp.where(quarter == g, moved, packed)
            es[layer, piece] = packed

    def unpack_edges(layer, piece, par):
        own = row * 32
        packed = er[layer, par, piece]
        first, size = PIECES[piece]
        for g in range(size // ROW_CHUNK):
            rows = pl.ds(first + g * ROW_CHUNK, ROW_CHUNK)
            both = yr[layer, par, rows, edge:]
            moved = pltpu.roll(packed, LANES - 32 * g, axis=1) if g else packed
            yr[layer, par, rows, :LANES] = both
            yr[layer, par, rows, edge:] = jnp.where(lane < own, both, moved)

    far = 3 * (1 - col // 2)
    near = 1 + lax.rem(col, 2)
    others = (far, 6 - col - far - near, near)

    def gather(layer, piece, par, j, src_col):
        at = (layer, par, src_col, pl.ds(*PIECES[piece]))
        return pltpu.make_async_remote_copy(
            src_ref=hblk.at[at], dst_ref=hblk.at[at],
            send_sem=a_send.at[layer, piece, j], recv_sem=a_recv.at[layer, par, piece, src_col],
            device_id={"col": others[j]}, device_id_type=MESH)

    def gather_start(layer, piece, par):
        for j in range(3):
            gather(layer, piece, par, j, col).start()

    def gather_wait_send(layer, par):
        for piece in range(len(PIECES)):
            for j in range(3):
                gather(layer, piece, par, j, col).wait_send()

    def gather_wait(layer, par):
        for piece in range(len(PIECES)):
            for j in range(3):
                gather(layer, piece, par, j, others[j]).wait_recv()

    def columns(i, start, size):
        return pl.ds(pl.multiple_of(owners[i] * tile_step + start, LANES), size)

    whole = ((0, width),)

    def dot_block(layer, par, weights, i, parts):
        total = None
        for k in range(4):
            rhs = [weights[k * n:(k + 1) * n, columns(i, *part)] for part in parts]
            rhs = rhs[0] if len(rhs) == 1 else jnp.concatenate(rhs, axis=1)
            part_sum = jnp.dot(hblk[layer, par, k, :, :n], rhs, preferred_element_type=F32)
            total = part_sum if total is None else total + part_sum
        return total

    def send_sums(layer, par, product, other, between):
        def block(i, parts):
            z, at = product(i, parts), 0
            for start, size in parts:
                zb[layer, i, :, start:start + size] = z[:, at:at + size] + other(i, start, size)
                at += size

        sent = 0
        for strip in STRIPS:
            block(0, strip)
            for _ in strip:
                d2d(layer, par, sent).start()
                sent += 1
        got = 0
        for j, strip in enumerate(STRIPS):
            block(1, strip)
            for _ in strip:
                d2d(layer, par, got).wait_recv()
                got += 1
            at = slice(strip[0][0], min(sum(strip[0]), edge))
            zb[layer, 1, :, at] = zb[layer, 1, :, at] + rd[layer, par, 0, :, at]
            if j == len(STRIPS) - 1:
                pack_edges(layer, par)
            ysum(layer, par, j).start()
        yedge(layer, par, 0).start()
        for piece in range(1, len(PIECES)):
            ysum(layer, par, len(STRIPS) + piece - 1).start()
            yedge(layer, par, piece).start()
        block(2, whole)
        d2d(layer, par, len(D2D_LANES)).start()
        between()
        block(3, whole)

    def cell_update(layer, piece, par, step):
        if piece == 0:
            d2d(layer, par, len(D2D_LANES)).wait_recv()
            for j in range(len(STRIPS)):
                ysum(layer, par, j).wait_recv()
        else:
            ysum(layer, par, len(STRIPS) + piece - 1).wait_recv()
        yedge(layer, par, piece).wait_recv()
        unpack_edges(layer, piece, par)
        span = pad_n + LANES
        unit = lax.broadcasted_iota(jnp.int32, (ROW_CHUNK, pad_n), 1)
        start0 = row * (4 * n - tile_step)
        first, size = PIECES[piece]
        for q in range(first, first + size, ROW_CHUNK):
            rows = pl.ds(q, ROW_CHUNK)
            gates = []
            for m in range(4):
                start = start0 + m * n
                tile = jnp.minimum(start // LANES, (width - span) // LANES)
                shift = start - tile * LANES
                at = pl.ds(pl.multiple_of(tile * LANES, LANES), span)
                z = zb[layer, 3, rows, at] + rd[layer, par, 1, rows, at] + yr[layer, par, rows, at]
                z = pltpu.roll(z, span - shift, axis=1)[:, :pad_n]
                gates.append(z + bias[layer, m:m + 1, :])
            c_new = (jax.nn.sigmoid(gates[1]) * cell[layer, rows, :]
                     + jax.nn.sigmoid(gates[0]) * jnp.tanh(gates[2]))
            cell[layer, rows, :] = c_new
            h_new = jnp.where(unit < n, jax.nn.sigmoid(gates[3]) * jnp.tanh(c_new), 0.0).astype(BF16)
            hblk[layer, par, col, rows, :] = h_new
            if layer == 1:
                h2_out[step, rows, :] = h_new[:, :n]

    def wait_sum_sends(layer, par):
        for j in range(len(D2D_LANES) + 1):
            d2d(layer, par, j).wait_send()
        for j in range(y_copies):
            ysum(layer, par, j).wait_send()
        for piece in range(len(PIECES)):
            yedge(layer, par, piece).wait_send()

    def finish(layer, piece, par, step, first):
        if piece == 0:
            @pl.when(jnp.logical_not(first))
            def _():
                gather_wait_send(layer, 1 - par)

        cell_update(layer, piece, par, step)
        gather_start(layer, piece, par)
        if piece == len(PIECES) - 1:
            wait_sum_sends(layer, par)

    def step_body(s, carry):
        par = lax.rem(s, 2)
        prev = 1 - par

        def finish_two():
            @pl.when(s >= 2)
            def _():
                finish(1, 1, par, s - 2, s == 2)

        @pl.when(s > 0)
        def _():
            gather_wait(0, prev)

        @pl.when(s < steps)
        def _():
            pin_copy(s).wait()

            @pl.when(s + 1 < steps)
            def _():
                pin_copy(s + 1).start()

            @pl.when(s == 0)
            def _():
                w_copies[0].wait()

            send_sums(0, par, lambda i, parts: dot_block(0, prev, w1, i, parts),
                      lambda i, start, size: pin[par, :, columns(i, start, size)], finish_two)

        @pl.when(s == steps)
        def _():
            finish_two()

        @pl.when(s >= 2)
        def _():
            finish(1, 2, par, s - 2, s == 2)

        @pl.when(s == 1)
        def _():
            w_copies[1].wait()
            w_copies[2].wait()

        @pl.when(s >= 1)
        def _():
            for i in range(4):
                zb[1, i] = dot_block(0, prev, w2i, i, whole)

        @pl.when(s == 0)
        def _():
            run_project(1)

        @pl.when(s < steps)
        def _():
            finish(0, 0, par, s, s == 0)

        def finish_one():
            @pl.when(s < steps)
            def _():
                finish(0, 1, par, s, s == 0)

        @pl.when(s >= 1)
        def _():
            @pl.when(s >= 2)
            def _():
                gather_wait(1, par)

            send_sums(1, prev, lambda i, parts: dot_block(1, par, w2r, i, parts),
                      lambda i, start, size: zb[1, i, :, start:start + size], finish_one)

        @pl.when(s == 0)
        def _():
            run_project(2)
            finish_one()

        @pl.when(s < steps)
        def _():
            finish(0, 2, par, s, s == 0)

        @pl.when(s == 0)
        def _():
            run_project(3)
            w_copies[2].start()

        @pl.when(jnp.logical_and(s >= 1, s < steps))
        def _():
            finish(1, 0, prev, s - 1, s == 1)

        return carry

    lax.fori_loop(0, steps + 1, step_body, 0)

    last = (steps - 1) % 2
    gather_wait_send(1, 1 - last)
    gather_wait_send(0, last)
    for piece in range(len(PIECES)):
        cell_update(1, piece, last, steps - 1)
    wait_sum_sends(1, last)
    c1_out[...] = cell[0, :, :n]
    c2_out[...] = cell[1, :, :n]


def solution(mesh):
    def local_program(seq_in, w_in1, w_rec1, b_gate1, w_in2, w_rec2, b_gate2, h_init, c_init):
        steps, batch, rows_dev = seq_in.shape
        cols_dev = w_in1.shape[1]
        n = b_gate1.shape[0] // 4
        pad_n = -(-n // LANES) * LANES
        width = -(-rows_dev // LANES) * LANES

        h0 = h_init.astype(BF16).reshape(2, batch, 4, n).transpose(0, 2, 1, 3)
        c0 = lax.dynamic_slice_in_dim(c_init, lax.axis_index("col") * n, n, axis=2)
        biases = (b_gate1.reshape(4, n), b_gate2.reshape(4, n))

        def kernel(*refs):
            lstm_kernel(steps, batch, n, rows_dev, cols_dev, width, pad_n, *refs)

        hbm = pl.BlockSpec(memory_space=pl.ANY)
        vmem = pl.BlockSpec(memory_space=pltpu.VMEM)
        dma = pltpu.SemaphoreType.DMA
        hops, pieces = len(D2D_LANES) + 1, len(PIECES)
        sends = len(STRIPS) + pieces - 1
        return pl.pallas_call(
            kernel,
            name="lstm_grid",
            out_shape=(jax.ShapeDtypeStruct((steps, batch, n), BF16),
                       jax.ShapeDtypeStruct((batch, n), F32),
                       jax.ShapeDtypeStruct((batch, n), F32),
                       jax.ShapeDtypeStruct((steps, batch, cols_dev), F32)),
            in_specs=[hbm] * 5 + [vmem] * 4,
            out_specs=(vmem, vmem, vmem, hbm),
            scratch_shapes=[
                pltpu.VMEM((rows_dev, cols_dev), BF16),
                pltpu.VMEM((rows_dev, cols_dev), BF16),
                pltpu.VMEM((rows_dev, cols_dev), BF16),
                pltpu.VMEM((2, GROUP, batch, rows_dev), BF16),
                pltpu.VMEM((2, batch, cols_dev), F32),
                pltpu.VMEM((2, batch, pad_n), F32),
                pltpu.VMEM((2, 8, pad_n), F32),
                pltpu.VMEM((2, 2, 4, batch, pad_n), BF16),
                pltpu.VMEM((2, 4, batch, width), F32),
                pltpu.VMEM((2, 2, 2, batch, width), F32),
                pltpu.VMEM((2, 2, batch, width), F32),
                pltpu.VMEM((2, len(PIECES), ROW_CHUNK, LANES), F32),
                pltpu.VMEM((2, 2, len(PIECES), ROW_CHUNK, LANES), F32),
                dma((3,)), dma((4,)), dma((2,)), dma((2,)), dma((2,)),
                dma((2, hops)), dma((2, 2, hops)),
                dma((2, sends)), dma((2, 2, sends)),
                dma((2, pieces)), dma((2, 2, pieces)),
                dma((2, pieces, 3)), dma((2, 2, pieces, 4)),
            ],
            compiler_params=pltpu.CompilerParams(
                collective_id=0, has_side_effects=True, vmem_limit_bytes=67043328),
        )(seq_in, w_in1, w_rec1, w_in2, w_rec2, h0, c0, *biases)[:3]

    row_spec = P(None, "dp", "row")
    weight_spec = P("row", "col")
    bias_spec = P(("col", "row"))
    seq_out_spec = P(None, "dp", ("row", "col"))
    cell_out_spec = P("dp", ("row", "col"))
    return jax.shard_map(
        local_program,
        mesh=mesh,
        in_specs=(row_spec, weight_spec, weight_spec, bias_spec, weight_spec, weight_spec, bias_spec, row_spec, row_spec),
        out_specs=(seq_out_spec, cell_out_spec, cell_out_spec),
        check_vma=False,
    )
```

```python
import jax
import jax.numpy as jnp
from jax import lax
from jax.experimental import pallas as pl
from jax.experimental.pallas import tpu as pltpu
from jax.sharding import PartitionSpec as P

MESH = pl.DeviceIdType.MESH
F32 = jnp.float32
BF16 = jnp.bfloat16
LANES = 128
ROW_CHUNK = 8
PIECES = ((0, 32), (32, 24), (56, 8))
STRIPS = (((128, 512),), ((640, 512),), ((1152, 384), (0, 128)))
D2D_LANES = tuple(part for strip in STRIPS for part in strip)
GROUP = 4


def lstm_kernel(steps, batch, n, rows_dev, cols_dev, width, pad_n,
                seq_hbm, w1i_hbm, w1_hbm, w2i_hbm, w2r_hbm, h0_ref, c0_ref, b1_ref, b2_ref,
                h2_out, c1_out, c2_out, pin_hbm,
                w1, w2i, w2r, xbuf, pin, cell, bias, hblk, zb, rd, yr, es, er,
                w_sem, wi_sem, x_sem, st_sem, pin_sem, d_send, d_recv, y_send, y_recv, e_send, e_recv, a_send, a_recv):
    row = lax.axis_index("row")
    col = lax.axis_index("col")
    core = lax.rem(row, 2)
    ypos = row // 2
    sibling = ypos * 2 + (1 - core)
    across = (1 - ypos) * 2 + core
    owners = ((1 - ypos) * 2 + (1 - core), across, sibling, row)
    tile_step = (n * 4) // LANES * LANES
    edge = width - LANES
    lane = lax.broadcasted_iota(jnp.int32, (ROW_CHUNK, LANES), 1)

    w_copies = [pltpu.make_async_copy(src, dst, w_sem.at[j])
                for j, (src, dst) in enumerate(((w1_hbm, w1), (w2i_hbm, w2i), (w2r_hbm, w2r)))]

    spans = 4

    def span_at(j):
        return pl.ds(pl.multiple_of(jnp.minimum(j * width, cols_dev - width), LANES), width)

    def w1i_copy(j):
        at = pl.ds(j * width, min(width, cols_dev - j * width))
        return pltpu.make_async_copy(w1i_hbm.at[:, at], w2r.at[:, at], wi_sem.at[j])

    def x_copy(g):
        return pltpu.make_async_copy(seq_hbm.at[pl.ds(g * GROUP, GROUP)], xbuf.at[g % 2], x_sem.at[g % 2])

    def stage_copy(g, j, slot):
        src = zb.at[1] if slot == 0 else rd.at[1].reshape(GROUP, batch, width)
        return pltpu.make_async_copy(src, pin_hbm.at[pl.ds(g * GROUP, GROUP), :, span_at(j)], st_sem.at[slot])

    def project(g):
        x_copy(g).wait()
        if (g + 1) * GROUP < steps:
            x_copy(g + 1).start()

        def pair(jj, carry):
            for slot in range(2):
                j = 2 * jj + slot

                @pl.when(jj > 0)
                def _():
                    stage_copy(g, j - 2, slot).wait()

                z = jnp.dot(xbuf[g % 2].reshape(GROUP * batch, rows_dev), w2r[:, span_at(j)], preferred_element_type=F32)
                if slot == 0:
                    zb[1] = z.reshape(GROUP, batch, width)
                else:
                    rd[1] = z.reshape(2, 2, batch, width)
                    @pl.when(jj > 0)
                    def _():
                        stage_copy(g, j - 1, 0).wait()
                stage_copy(g, j, slot).start()
            return carry

        return pair

    def run_project(g):
        lax.fori_loop(0, spans // 2, project(g), 0)
        stage_copy(g, spans - 1, 1).wait()

    x_copy(0).start()
    for j in range(spans):
        w1i_copy(j).start()

    def pin_copy(step):
        slot = lax.rem(step, 2)
        return pltpu.make_async_copy(pin_hbm.at[step], pin.at[slot], pin_sem.at[slot])

    barrier = pltpu.get_barrier_semaphore()
    for peer_row in (sibling, across):
        pl.semaphore_signal(barrier, inc=1, device_id={"row": peer_row}, device_id_type=MESH)
    for j in (1, 2, 3):
        pl.semaphore_signal(barrier, inc=1, device_id={"col": lax.rem(col + j, 4)}, device_id_type=MESH)

    for layer in range(2):
        cell[layer] = jnp.zeros((batch, pad_n), F32)
        bias[layer] = jnp.zeros((8, pad_n), F32)
        for k in range(4):
            own = slice(k * n, (k + 1) * n)
            hblk[layer, 1, k, :, :n] = h0_ref[layer, :, own].astype(BF16)
            bias[layer, k:k + 1, :n] = (b1_ref, b2_ref)[layer][:, own]

            @pl.when(col == k)
            def _(own=own, layer=layer):
                cell[layer, :, :n] = c0_ref[layer, :, own]
    first_pair = project(0)
    for jj in range(spans // 2):
        w1i_copy(2 * jj).wait()
        w1i_copy(2 * jj + 1).wait()
        first_pair(jj, 0)
        w_copies[jj].start()
    stage_copy(0, spans - 1, 1).wait()
    pin_copy(0).start()
    pl.semaphore_wait(barrier, 5)

    def d2d(layer, par, j):
        if j < len(D2D_LANES):
            at = pl.ds(*D2D_LANES[j])
            src, dst = zb.at[layer, 0, :, at], rd.at[layer, par, 0, :, at]
        else:
            src, dst = zb.at[layer, 2], rd.at[layer, par, 1]
        return pltpu.make_async_remote_copy(
            src_ref=src, dst_ref=dst, send_sem=d_send.at[layer, j], recv_sem=d_recv.at[layer, par, j],
            device_id={"row": sibling}, device_id_type=MESH)

    def ysum(layer, par, j):
        if j < len(STRIPS):
            at = (pl.ds(*PIECES[0]), pl.ds(*STRIPS[j][0]))
        else:
            at = (pl.ds(*PIECES[j - len(STRIPS) + 1]), pl.ds(LANES, edge))
        return pltpu.make_async_remote_copy(
            src_ref=zb.at[(layer, 1) + at], dst_ref=yr.at[(layer, par) + at],
            send_sem=y_send.at[layer, j], recv_sem=y_recv.at[layer, par, j],
            device_id={"row": across}, device_id_type=MESH)

    def yedge(layer, par, piece):
        return pltpu.make_async_remote_copy(
            src_ref=es.at[layer, piece], dst_ref=er.at[layer, par, piece],
            send_sem=e_send.at[layer, piece], recv_sem=e_recv.at[layer, par, piece],
            device_id={"row": across}, device_id_type=MESH)

    y_copies = len(STRIPS) + len(PIECES) - 1

    def pack_edges(layer, par):
        own = across * 32
        quarter = jnp.bitwise_and(jnp.right_shift(lane, 5) + 4 - across, 3)
        for piece, (first, size) in enumerate(PIECES):
            packed = None
            for g in range(size // ROW_CHUNK):
                rows = pl.ds(first + g * ROW_CHUNK, ROW_CHUNK)
                head = zb[layer, 1, rows, :LANES] + rd[layer, par, 0, rows, :LANES]
                tail = zb[layer, 1, rows, edge:] + rd[layer, par, 0, rows, edge:]
                zb[layer, 1, rows, edge:] = jnp.where(lane >= own, head, tail)
                moved = pltpu.roll(tail, 32 * g, axis=1) if g else tail
                packed = moved if packed is None else jnp.where(quarter == g, moved, packed)
            es[layer, piece] = packed

    def unpack_edges(layer, piece, par):
        own = row * 32
        packed = er[layer, par, piece]
        first, size = PIECES[piece]
        for g in range(size // ROW_CHUNK):
            rows = pl.ds(first + g * ROW_CHUNK, ROW_CHUNK)
            both = yr[layer, par, rows, edge:]
            moved = pltpu.roll(packed, LANES - 32 * g, axis=1) if g else packed
            yr[layer, par, rows, :LANES] = both
            yr[layer, par, rows, edge:] = jnp.where(lane < own, both, moved)

    far = 3 * (1 - col // 2)
    near = 1 + lax.rem(col, 2)
    others = (far, 6 - col - far - near, near)

    def gather(layer, piece, par, j, src_col):
        at = (layer, par, src_col, pl.ds(*PIECES[piece]))
        return pltpu.make_async_remote_copy(
            src_ref=hblk.at[at], dst_ref=hblk.at[at],
            send_sem=a_send.at[layer, piece, j], recv_sem=a_recv.at[layer, par, piece, src_col],
            device_id={"col": others[j]}, device_id_type=MESH)

    def gather_start(layer, piece, par):
        for j in range(3):
            gather(layer, piece, par, j, col).start()

    def gather_wait_send(layer, par):
        for piece in range(len(PIECES)):
            for j in range(3):
                gather(layer, piece, par, j, col).wait_send()

    def gather_wait(layer, par):
        for piece in range(len(PIECES)):
            for j in range(3):
                gather(layer, piece, par, j, others[j]).wait_recv()

    def columns(i, start, size):
        return pl.ds(pl.multiple_of(owners[i] * tile_step + start, LANES), size)

    whole = ((0, width),)

    def dot_block(layer, par, weights, i, parts):
        total = None
        for k in range(4):
            rhs = [weights[k * n:(k + 1) * n, columns(i, *part)] for part in parts]
            rhs = rhs[0] if len(rhs) == 1 else jnp.concatenate(rhs, axis=1)
            part_sum = jnp.dot(hblk[layer, par, k, :, :n], rhs, preferred_element_type=F32)
            total = part_sum if total is None else total + part_sum
        return total

    def send_sums(layer, par, product, other, between):
        def block(i, parts):
            z, at = product(i, parts), 0
            for start, size in parts:
                zb[layer, i, :, start:start + size] = z[:, at:at + size] + other(i, start, size)
                at += size

        sent = 0
        for strip in STRIPS:
            block(0, strip)
            for _ in strip:
                d2d(layer, par, sent).start()
                sent += 1
        got = 0
        for j, strip in enumerate(STRIPS):
            block(1, strip)
            for _ in strip:
                d2d(layer, par, got).wait_recv()
                got += 1
            at = slice(strip[0][0], min(sum(strip[0]), edge))
            zb[layer, 1, :, at] = zb[layer, 1, :, at] + rd[layer, par, 0, :, at]
            if j == len(STRIPS) - 1:
                pack_edges(layer, par)
            ysum(layer, par, j).start()
            if j == 0:
                between(0)
        yedge(layer, par, 0).start()
        for piece in range(1, len(PIECES)):
            ysum(layer, par, len(STRIPS) + piece - 1).start()
            yedge(layer, par, piece).start()
        block(2, whole)
        d2d(layer, par, len(D2D_LANES)).start()
        between(1)
        block(3, whole)
        between(2)

    def cell_update(layer, piece, par, step):
        if piece == 0:
            d2d(layer, par, len(D2D_LANES)).wait_recv()
            for j in range(len(STRIPS)):
                ysum(layer, par, j).wait_recv()
        else:
            ysum(layer, par, len(STRIPS) + piece - 1).wait_recv()
        yedge(layer, par, piece).wait_recv()
        unpack_edges(layer, piece, par)
        span = pad_n + LANES
        unit = lax.broadcasted_iota(jnp.int32, (ROW_CHUNK, pad_n), 1)
        start0 = row * (4 * n - tile_step)
        first, size = PIECES[piece]
        for q in range(first, first + size, ROW_CHUNK):
            rows = pl.ds(q, ROW_CHUNK)
            gates = []
            for m in range(4):
                start = start0 + m * n
                tile = jnp.minimum(start // LANES, (width - span) // LANES)
                shift = start - tile * LANES
                at = pl.ds(pl.multiple_of(tile * LANES, LANES), span)
                z = zb[layer, 3, rows, at] + rd[layer, par, 1, rows, at] + yr[layer, par, rows, at]
                z = pltpu.roll(z, span - shift, axis=1)[:, :pad_n]
                gates.append(z + bias[layer, m:m + 1, :])
            c_new = (jax.nn.sigmoid(gates[1]) * cell[layer, rows, :]
                     + jax.nn.sigmoid(gates[0]) * jnp.tanh(gates[2]))
            cell[layer, rows, :] = c_new
            h_new = jnp.where(unit < n, jax.nn.sigmoid(gates[3]) * jnp.tanh(c_new), 0.0).astype(BF16)
            hblk[layer, par, col, rows, :] = h_new
            if layer == 1:
                h2_out[step, rows, :] = h_new[:, :n]

    def wait_sum_sends(layer, par):
        for j in range(len(D2D_LANES) + 1):
            d2d(layer, par, j).wait_send()
        for j in range(y_copies):
            ysum(layer, par, j).wait_send()
        for piece in range(len(PIECES)):
            yedge(layer, par, piece).wait_send()

    def finish(layer, piece, par, step, first):
        if piece == 0:
            @pl.when(jnp.logical_not(first))
            def _():
                gather_wait_send(layer, 1 - par)

        cell_update(layer, piece, par, step)
        gather_start(layer, piece, par)
        if piece == len(PIECES) - 1:
            wait_sum_sends(layer, par)

    def step_body(s, carry):
        par = lax.rem(s, 2)
        prev = 1 - par

        def finish_two(piece):
            @pl.when(s >= 2)
            def _():
                finish(1, piece, par, s - 2, s == 2)

        def finish_one(piece):
            @pl.when(s < steps)
            def _():
                finish(0, piece, par, s, s == 0)

        @pl.when(s > 0)
        def _():
            gather_wait(0, prev)

        @pl.when(s < steps)
        def _():
            @pl.when(s == 0)
            def _():
                w_copies[0].wait()

            @pl.when(s + 1 < steps)
            def _():
                pin_copy(s + 1).start()

            pin_copy(s).wait()
            send_sums(0, par, lambda i, parts: dot_block(0, prev, w1, i, parts),
                      lambda i, start, size: pin[par, :, columns(i, start, size)], finish_two)

        @pl.when(s == steps)
        def _():
            for piece in range(len(PIECES)):
                finish_two(piece)

        @pl.when(s == 1)
        def _():
            w_copies[1].wait()
            w_copies[2].wait()

        @pl.when(s >= 1)
        def _():
            for i in range(4):
                zb[1, i] = dot_block(0, prev, w2i, i, whole)

            @pl.when(s >= 2)
            def _():
                gather_wait(1, par)

            send_sums(1, prev, lambda i, parts: dot_block(1, par, w2r, i, parts),
                      lambda i, start, size: zb[1, i, :, start:start + size], finish_one)

        @pl.when(s == 0)
        def _():
            run_project(1)
            finish_one(0)
            run_project(2)
            finish_one(1)
            finish_one(2)
            run_project(3)
            w_copies[2].start()

        return carry

    lax.fori_loop(0, steps + 1, step_body, 0)

    last = (steps - 1) % 2
    gather_wait_send(1, 1 - last)
    gather_wait_send(0, last)
    for piece in range(len(PIECES)):
        cell_update(1, piece, last, steps - 1)
    wait_sum_sends(1, last)
    c1_out[...] = cell[0, :, :n]
    c2_out[...] = cell[1, :, :n]


def solution(mesh):
    def local_program(seq_in, w_in1, w_rec1, b_gate1, w_in2, w_rec2, b_gate2, h_init, c_init):
        steps, batch, rows_dev = seq_in.shape
        cols_dev = w_in1.shape[1]
        n = b_gate1.shape[0] // 4
        pad_n = -(-n // LANES) * LANES
        width = -(-rows_dev // LANES) * LANES

        def kernel(*refs):
            lstm_kernel(steps, batch, n, rows_dev, cols_dev, width, pad_n, *refs)

        hbm = pl.BlockSpec(memory_space=pl.ANY)
        vmem = pl.BlockSpec(memory_space=pltpu.VMEM)
        dma = pltpu.SemaphoreType.DMA
        hops, pieces = len(D2D_LANES) + 1, len(PIECES)
        sends = len(STRIPS) + pieces - 1
        return pl.pallas_call(
            kernel,
            name="lstm_grid",
            out_shape=(jax.ShapeDtypeStruct((steps, batch, n), BF16),
                       jax.ShapeDtypeStruct((batch, n), F32),
                       jax.ShapeDtypeStruct((batch, n), F32),
                       jax.ShapeDtypeStruct((steps, batch, cols_dev), F32)),
            in_specs=[hbm] * 5 + [vmem] * 4,
            out_specs=(vmem, vmem, vmem, hbm),
            scratch_shapes=[
                pltpu.VMEM((rows_dev, cols_dev), BF16),
                pltpu.VMEM((rows_dev, cols_dev), BF16),
                pltpu.VMEM((rows_dev, cols_dev), BF16),
                pltpu.VMEM((2, GROUP, batch, rows_dev), BF16),
                pltpu.VMEM((2, batch, cols_dev), F32),
                pltpu.VMEM((2, batch, pad_n), F32),
                pltpu.VMEM((2, 8, pad_n), F32),
                pltpu.VMEM((2, 2, 4, batch, pad_n), BF16),
                pltpu.VMEM((2, 4, batch, width), F32),
                pltpu.VMEM((2, 2, 2, batch, width), F32),
                pltpu.VMEM((2, 2, batch, width), F32),
                pltpu.VMEM((2, len(PIECES), ROW_CHUNK, LANES), F32),
                pltpu.VMEM((2, 2, len(PIECES), ROW_CHUNK, LANES), F32),
                dma((3,)), dma((4,)), dma((2,)), dma((2,)), dma((2,)),
                dma((2, hops)), dma((2, 2, hops)),
                dma((2, sends)), dma((2, 2, sends)),
                dma((2, pieces)), dma((2, 2, pieces)),
                dma((2, pieces, 3)), dma((2, 2, pieces, 4)),
            ],
            compiler_params=pltpu.CompilerParams(
                collective_id=0, has_side_effects=True, vmem_limit_bytes=67043328),
        )(seq_in, w_in1, w_rec1, w_in2, w_rec2, h_init, c_init, b_gate1[None], b_gate2[None])[:3]

    row_spec = P(None, "dp", "row")
    weight_spec = P("row", "col")
    bias_spec = P(("col", "row"))
    seq_out_spec = P(None, "dp", ("row", "col"))
    cell_out_spec = P("dp", ("row", "col"))
    return jax.shard_map(
        local_program,
        mesh=mesh,
        in_specs=(row_spec, weight_spec, weight_spec, bias_spec, weight_spec, weight_spec, bias_spec, row_spec, row_spec),
        out_specs=(seq_out_spec, cell_out_spec, cell_out_spec),
        check_vma=False,
    )
```
